512 devices in a mesh: seq: 64 (over y, z), head: 4 (over x), req: 2 (over core).
Axes of the slice: x: 4, y: 8, z: 8, core: 2. Of those that a mesh axis runs over, the one named last changes fastest.
Arguments:
- queries: bfloat16 [8, 512, 128], P('req', ('head', 'seq')), may hold values from -256 to 256
- key_codes: bfloat16 [8, 8, 32768, 128], P('req', 'head', 'seq'), may hold values from -448 to 448
- key_scale: float32 [8, 8, 512], P('req', 'head', 'seq'), may hold values from 0.01 to 0.1
- value_codes: bfloat16 [8, 8, 32768, 128], P('req', 'head', 'seq'), may hold values from -192 to 192
- value_scale: float32 [8, 8, 512], P('req', 'head', 'seq'), may hold values from 0.01 to 0.06
- out_weight: bfloat16 [16384, 16384], P('head', 'seq'), may hold values from -0.1875 to 0.1875
- ctx_len: int32 [8], P('req'), may hold values from 8192 to 32768, as said below
- start_shard: int32 [8], P('req'), may hold values from 0 to 63
- draft_depth: int32 [8, 4], P('req'), may hold values from 0 to 3
Outputs:
- projected: bfloat16 [4, 8, 16384], P('head', 'req', 'seq')
The draws below stay inside these ranges and needn't reach their ends.
Inputs may be any that keep to these rules, and one draw needn't show every extreme that they name: `ctx_len`: at least one request has exactly 32768 positions.
All inputs are finite; a program needn't handle non-finite values.
Results may differ from the reference program's by a relative error of at most 0.0057.
Values may be sent and summed in bfloat16 or wider, within the bound.
A program may use at most 64 MiB of HBM per device.

```python
import math
import jax
import jax.numpy as jnp
from jax import lax

D = 16384
QHEADS = 128
KVH = 8
HD = 128
DRAFT = 4
BLK = 64
KV_DEV = 512
REQS = 8
CTX = 32768
N_SEQ = 64


def world(key):
    parts = jax.random.split(key, 8)
    shard_count = CTX // KV_DEV
    lengths = jax.random.randint(parts[0], (REQS,), CTX // 4, CTX + 1)
    longest = jax.random.randint(parts[1], (), 0, REQS)
    lengths = jnp.where(jnp.arange(REQS) == longest, CTX, lengths).astype(jnp.int32)
    starts = jax.random.randint(parts[2], (REQS,), 0, shard_count)
    last_pick = jax.random.randint(parts[6], (), 0, REQS)
    first_pick = jnp.mod(last_pick + 1 + jax.random.randint(parts[7], (), 0, REQS - 1), REQS)
    request_ids = jnp.arange(REQS)
    starts = jnp.where(request_ids == last_pick, shard_count - 1, starts)
    starts = jnp.where(request_ids == first_pick, 0, starts).astype(jnp.int32)
    depths = jax.random.randint(parts[3], (REQS, DRAFT), 0, DRAFT).astype(jnp.int32)
    codes = jnp.clip(32.0 * jax.random.normal(parts[4], (REQS, KVH, CTX, HD), jnp.float32), -448.0, 448.0).astype(jnp.bfloat16)
    scales = jnp.exp(jax.random.uniform(parts[5], (REQS, KVH, CTX // BLK), jnp.float32, math.log(0.01), math.log(0.1)))
    return (lengths, starts, depths, codes, scales)


def draw_ctx_len(key, part):
    return world(key)[0]


def draw_start_shard(key, part):
    return world(key)[1]


def draw_draft_depth(key, part):
    return world(key)[2]


def draw_key_codes(key, part):
    return world(key)[3]


def draw_key_scale(key, part):
    return world(key)[4]


def draw_queries(key, part):
    lengths, starts, depths, codes, scales = world(key)
    extra = jax.random.split(jax.random.fold_in(key, 91), 3)
    group = QHEADS // KVH
    shard_count = CTX // KV_DEV
    own_pos = lengths[:, None] - DRAFT + depths
    tie_pos = jax.random.randint(extra[0], (REQS, DRAFT), 0, 1 << 20) % (lengths[:, None] - DRAFT)

    def fetch(position):
        where_at = jnp.mod(starts[:, None] + position // KV_DEV, shard_count) * KV_DEV + position % KV_DEV
        picked = jnp.take_along_axis(codes, where_at[:, None, :, None], axis=2).astype(jnp.float32)
        factor = jnp.take_along_axis(scales, (where_at // BLK)[:, None, :], axis=2)
        return picked * factor[..., None]
    own = fetch(own_pos)
    tie = fetch(tie_pos)
    root = math.sqrt(HD)
    g_one = (jnp.sum(own * own, axis=-1) / root)[:, :, None, :]
    g_mix = (jnp.sum(own * tie, axis=-1) / root)[:, :, None, :]
    g_two = (jnp.sum(tie * tie, axis=-1) / root)[:, :, None, :]
    strength = jax.random.uniform(extra[1], (REQS, KVH, group, DRAFT), jnp.float32, 3.0, 8.0)
    second = jnp.where(strength > 0.0, strength - 2.0, 0.0)
    determinant = g_one * g_two - g_mix * g_mix
    alpha = (g_two * strength - g_mix * second) / determinant
    beta = (g_one * second - g_mix * strength) / determinant
    unit_one = own / jnp.sqrt(jnp.sum(own * own, axis=-1, keepdims=True))
    remainder = tie - jnp.sum(tie * unit_one, axis=-1, keepdims=True) * unit_one
    unit_two = remainder / jnp.sqrt(jnp.sum(remainder * remainder, axis=-1, keepdims=True))
    unit_one = unit_one[:, :, None]
    unit_two = unit_two[:, :, None]
    noise = jax.random.normal(extra[2], (REQS, KVH, group, DRAFT, HD), jnp.float32)
    noise = noise - jnp.sum(noise * unit_one, axis=-1, keepdims=True) * unit_one
    noise = noise - jnp.sum(noise * unit_two, axis=-1, keepdims=True) * unit_two
    values = noise + alpha[..., None] * own[:, :, None] + beta[..., None] * tie[:, :, None]
    return jnp.clip(values, -256.0, 256.0).reshape(REQS, QHEADS * DRAFT, HD).astype(jnp.bfloat16)


def block_scale(stream_key, extent, cuts, smallest, high):
    loudness, own = 1.0, jax.random.fold_in(stream_key, 6)
    for dim, blocks in cuts:
        heights = jnp.exp(jax.random.uniform(jax.random.fold_in(own, dim), (blocks,), jnp.float32, smallest / len(cuts), high / len(cuts)))
        loudness = loudness * jnp.repeat(heights, extent[dim] // blocks).reshape([-1 if axis == dim else 1 for axis in range(len(extent))])
    return loudness


def scatter_about(key, extent, scale, limit, shards=(), kind=jnp.bfloat16):
    drawn = jax.random.normal(key, extent, jnp.float32) * scale
    if len(shards) > 0:
        drawn = block_scale(key, extent, shards, -0.22, 0.18) * drawn
    return jnp.clip(drawn, min=-limit, max=limit).astype(kind)


def setup_inputs(seed: int = 0) -> dict:
    seeds = jax.random.split(jax.random.key(seed), 10)
    return {
        "queries": draw_queries(jax.random.fold_in(seeds[9], 71), 0),
        "key_codes": draw_key_codes(jax.random.fold_in(seeds[9], 71), 0),
        "key_scale": draw_key_scale(jax.random.fold_in(seeds[9], 71), 0),
        "value_codes": scatter_about(seeds[3], (REQS, KVH, CTX, HD), 32.0, 192.0, ((0, 2), (1, 4), (2, 64))),
        "value_scale": jnp.clip(jnp.exp(math.log(0.06) - 1.7917595 * jax.random.uniform(seeds[4], (REQS, KVH, CTX // BLK), jnp.float32) ** block_scale(seeds[4], (REQS, KVH, CTX // BLK), ((0, 2), (1, 4), (2, 64)), -0.2, 0.2)), 0.01, 0.06),
        "out_weight": scatter_about(seeds[5], (QHEADS * HD, D), (KVH * HD) ** -0.5, 0.1875, ((0, 4), (1, 64))),
        "ctx_len": draw_ctx_len(jax.random.fold_in(seeds[9], 71), 0),
        "start_shard": draw_start_shard(jax.random.fold_in(seeds[9], 71), 0),
        "draft_depth": draw_draft_depth(jax.random.fold_in(seeds[9], 71), 0),
    }


NEG_FLOOR = -1e+30

def combine_state(first, second):
    top = jnp.maximum(first[0], second[0])
    early = jnp.exp(first[0] - top)
    later = jnp.exp(second[0] - top)
    return (top, first[1] * early + second[1] * later, first[2] * early[..., None] + second[2] * later[..., None])

def shard_partial(block_q, key_block, key_tok, value_block, value_tok, positions, limits):
    raw = jnp.einsum('rhqd,rhkd->rhqk', block_q.astype(jnp.float32), key_block.astype(jnp.float32))
    scores = raw * (key_tok[:, :, None, :] * (1.0 / math.sqrt(HD)))
    visible = positions[:, None, None, :] <= limits[:, None, :, None]
    masked = jnp.where(visible, scores, NEG_FLOOR)
    top = lax.optimization_barrier(jnp.max(masked, axis=3))
    weights = jnp.where(visible, jnp.exp(masked - top[..., None]), 0.0)
    total = lax.optimization_barrier(jnp.sum(weights, axis=3))
    scaled = (weights * value_tok[:, :, None, :]).astype(jnp.bfloat16)
    acc = jnp.einsum('rhqk,rhkd->rhqd', scaled.astype(jnp.float32), value_block.astype(jnp.float32))
    return (top, total, acc)

def reference(queries, key_codes, key_scale, value_codes, value_scale, out_weight, ctx_len, start_shard, draft_depth):
    group_rows = QHEADS // KVH * DRAFT
    grouped = queries.reshape(REQS, KVH, group_rows, HD)
    draft_of = jnp.arange(group_rows, dtype=jnp.int32) % DRAFT
    limits = (ctx_len - DRAFT)[:, None] + draft_depth[:, draft_of]
    per_shard = KV_DEV // BLK

    def visit(state, shard):
        key_block = lax.dynamic_slice_in_dim(key_codes, shard * KV_DEV, KV_DEV, 2)
        value_block = lax.dynamic_slice_in_dim(value_codes, shard * KV_DEV, KV_DEV, 2)
        key_tok = jnp.repeat(lax.dynamic_slice_in_dim(key_scale, shard * per_shard, per_shard, 2), BLK, axis=2)
        value_tok = jnp.repeat(lax.dynamic_slice_in_dim(value_scale, shard * per_shard, per_shard, 2), BLK, axis=2)
        positions = jnp.mod(shard - start_shard, N_SEQ)[:, None] * KV_DEV + jnp.arange(KV_DEV, dtype=jnp.int32)[None, :]
        part = shard_partial(grouped, key_block, key_tok, value_block, value_tok, positions, limits)
        return (combine_state(state, part), None)
    start_state = (jnp.full((REQS, KVH, group_rows), NEG_FLOOR, jnp.float32), jnp.zeros((REQS, KVH, group_rows), jnp.float32), jnp.zeros((REQS, KVH, group_rows, HD), jnp.float32))
    final, unused = lax.scan(visit, start_state, jnp.arange(N_SEQ, dtype=jnp.int32))
    attention = (final[2] / final[1][..., None]).astype(jnp.bfloat16)
    arranged = attention.reshape(REQS, QHEADS, DRAFT, HD)
    flat = jnp.transpose(arranged, (2, 0, 1, 3)).reshape(DRAFT * REQS, QHEADS * HD)
    result = jnp.dot(flat, out_weight, preferred_element_type=jnp.float32)
    return result.reshape(DRAFT, REQS, D).astype(jnp.bfloat16)
```

```python
import math

import jax
import jax.numpy as jnp
from jax import lax
from jax.experimental import pallas as pl
from jax.experimental.pallas import tpu as pltpu
from jax.sharding import Mesh
from jax.sharding import PartitionSpec as P

QHEADS = 128
KVH = 8
HD = 128
DRAFT = 4
BLK = 64
SEQ = ("seq_0", "seq_1")
HEAD_SEQ = ("head", "seq_0", "seq_1")
MESH = pl.DeviceIdType.MESH

N = 8
NX = 4
R = 4
KV = 2
ROWS = 64
KEYS = 512
NEG = -1e30
FLOOR = -1e29
ORDER = (4, 3, 5, 2, 6, 1, 7)
FIRST = ("seq_1", "seq_0")
SECOND = ("seq_0", "seq_1")


def peer(axis, k, size):
    return lax.rem(lax.axis_index(axis) + k, size)


def f32(x):
    return x.astype(jnp.float32)


def bf16(x):
    return x.astype(jnp.bfloat16)


def kernel(
    q_hbm, k_hbm, ks_hbm, v_hbm, vs_hbm, w_hbm, ctx_hbm, start_hbm, depth_hbm,
    out_ref,
    q0, q1, qf, kbuf, vbuf, wbuf, ks, vs, ctx, start, depth,
    sacc, sst, racc, rst, cacc, cst, dacc, dst, att, ybuf, xbuf,
    lsem, ssem, rsem, xs, xr,
):
    y = lax.axis_index("seq_0")
    z = lax.axis_index("seq_1")
    x = lax.axis_index("head")
    line = {"seq_0": y, "seq_1": z}
    here = y * N + z

    barrier = pltpu.get_barrier_semaphore()
    for axis in SEQ:
        for k in ORDER:
            pl.semaphore_signal(barrier, inc=1, device_id={axis: peer(axis, k, N)}, device_id_type=MESH)
    for k in (2, 1, 3):
        pl.semaphore_signal(barrier, inc=1, device_id={"head": peer("head", k, NX)}, device_id_type=MESH)

    qc0 = pltpu.make_async_copy(q_hbm.at[pl.ds(0, 2)], q0.at[:, z], lsem.at[0])
    qc1 = pltpu.make_async_copy(q_hbm.at[pl.ds(2, 2)], q1.at[:, y], lsem.at[1])
    qc0.start()
    qc1.start()
    small = [
        pltpu.make_async_copy(a, b, lsem.at[2 + i])
        for i, (a, b) in enumerate(
            ((ks_hbm, ks), (vs_hbm, vs), (ctx_hbm, ctx), (start_hbm, start), (depth_hbm, depth))
        )
    ]
    for c in small:
        c.start()
    kc = pltpu.make_async_copy(k_hbm, kbuf, lsem.at[7])
    vc = pltpu.make_async_copy(v_hbm, vbuf, lsem.at[8])
    wc = pltpu.make_async_copy(w_hbm, wbuf, lsem.at[9])
    kc.start()
    vc.start()
    wc.start()
    qc0.wait()
    qc1.wait()
    pl.semaphore_wait(barrier, 2 * (N - 1) + NX - 1)

    sent = []

    def send(src, dst, slot, axis, k):
        copy = pltpu.make_async_remote_copy(
            src_ref=src, dst_ref=dst, send_sem=ssem.at[slot, k - 1], recv_sem=rsem.at[slot, k - 1],
            device_id={axis: peer(axis, k, N)}, device_id_type=MESH,
        )
        copy.start()
        sent.append(copy)

    def arrived(src, dst, slot, axis, k):
        pltpu.make_async_remote_copy(
            src_ref=src, dst_ref=dst, send_sem=ssem.at[slot, k - 1], recv_sem=rsem.at[slot, k - 1],
            device_id={axis: peer(axis, k, N)}, device_id_type=MESH,
        ).wait_recv()

    for k in ORDER:
        send(q0.at[:, z], q0.at[:, z], 0, "seq_1", k)
        send(q1.at[:, y], q1.at[:, y], 1, "seq_0", k)
    for k in ORDER[::-1]:
        zz = peer("seq_1", N - k, N)
        arrived(q0.at[:, z], q0.at[:, zz], 0, "seq_1", k)
    for k in ORDER:
        send(q0, qf.at[pl.ds(0, 2), y], 2, "seq_0", k)
    for k in ORDER[::-1]:
        yy = peer("seq_0", N - k, N)
        arrived(q1.at[:, y], q1.at[:, yy], 1, "seq_0", k)
    for k in ORDER:
        send(q1, qf.at[pl.ds(2, 2), :, z], 3, "seq_1", k)
    qf[0:2, y] = q0[...]
    qf[2:4, :, z] = q1[...]
    for c in small:
        c.wait()

    lane_key = lax.broadcasted_iota(jnp.int32, (ROWS, KEYS), 1)
    lane_row = lax.broadcasted_iota(jnp.int32, (1, HD), 1)
    draft = lax.rem(lax.broadcasted_iota(jnp.int32, (ROWS, 1), 0), DRAFT)
    lane = lax.broadcasted_iota(jnp.int32, (ROWS, HD), 1)
    factor = math.log2(math.e) / math.sqrt(HD)

    def scale_row(ref, r, h, by):
        tiles = []
        for j in range(KEYS // HD):
            tiles.append(jnp.where(lane_row < BLK, ref[r, h, 2 * j] * by, ref[r, h, 2 * j + 1] * by))
        return jnp.concatenate(tiles, axis=1)

    kc.wait()
    vc.wait()
    for half in range(2):
        if half == 0:
            for k in ORDER[::-1]:
                arrived(q0, qf.at[pl.ds(0, 2), peer("seq_0", N - k, N)], 2, "seq_0", k)
        else:
            for k in ORDER[::-1]:
                arrived(q1, qf.at[pl.ds(2, 2), :, peer("seq_1", N - k, N)], 3, "seq_1", k)
        axis = FIRST[half]
        stats = jnp.zeros((ROWS, HD), jnp.float32)
        for r2 in range(2):
            r = half * 2 + r2
            offset = lax.rem(here - start[r] + N * N, N * N) * KEYS
            base = ctx[r] - DRAFT - offset
            limit = jnp.full((ROWS, 1), base + depth[r, 0], jnp.int32)
            for t in range(1, DRAFT):
                limit = jnp.where(draft == t, base + depth[r, t], limit)
            visible = lane_key <= limit
            accs = []
            for h in range(KV):
                rows = qf[r, 4 * h : 4 * h + 4].reshape(ROWS, HD)
                raw = lax.dot_general(
                    rows, kbuf[r, h], (((1,), (1,)), ((), ())), preferred_element_type=jnp.float32
                )
                score = jnp.where(visible, raw * scale_row(ks, r, h, factor), NEG)
                top = jnp.maximum(jnp.max(score, axis=1, keepdims=True), FLOOR)
                weight = jnp.exp2(score - top)
                total = jnp.sum(weight, axis=1, keepdims=True)
                scaled = bf16(weight * scale_row(vs, r, h, 1.0))
                accs.append(jnp.dot(scaled, vbuf[r, h], preferred_element_type=jnp.float32))
                c = r2 * KV + h
                stats = jnp.where(lane == c, top, stats)
                stats = jnp.where(lane == BLK + c, total, stats)
            for o in range(N):
                part = jnp.concatenate([a[8 * o : 8 * o + 8] for a in accs], axis=0)
                sacc[half, o, r2] = bf16(part)
        for o in range(N):
            sst[half, o] = stats[8 * o : 8 * o + 8]
        me = line[axis]
        for k in ORDER:
            to = peer(axis, k, N)
            send(sacc.at[half, to], racc.at[half, me], 4 + half, axis, k)
            send(sst.at[half, to], rst.at[half, me], 6 + half, axis, k)
        racc[half, me] = sacc[half, me]
        rst[half, me] = sst[half, me]

    small_lane = lax.broadcasted_iota(jnp.int32, (8, HD), 1)

    def combine(accs, stats, half, last):
        st = [stats[half, k] for k in range(N)]
        top = st[0]
        for s in st[1:]:
            top = jnp.maximum(top, s)
        fs = [jnp.exp2(s - top) for s in st]
        total = jnp.zeros((8, HD), jnp.float32)
        for s, f in zip(st, fs):
            total = total + pltpu.roll(s, BLK, 1) * f
        if last:
            inv = 1.0 / total
            fs = [f * inv for f in fs]
        outs = []
        for r2 in range(2):
            acc = jnp.zeros((16, HD), jnp.float32)
            for k in range(N):
                w = jnp.concatenate(
                    [jnp.broadcast_to(fs[k][:, r2 * KV + h : r2 * KV + h + 1], (8, HD)) for h in range(KV)],
                    axis=0,
                )
                acc = acc + f32(accs[half, k, r2]) * w
            outs.append(bf16(acc))
        return outs, jnp.where(small_lane < BLK, top, pltpu.roll(total, BLK, 1))

    for half in range(2):
        axis = FIRST[half]
        for k in ORDER[::-1]:
            frm = peer(axis, N - k, N)
            arrived(sacc.at[half, 0], racc.at[half, frm], 4 + half, axis, k)
            arrived(sst.at[half, 0], rst.at[half, frm], 6 + half, axis, k)
        outs, st = combine(racc, rst, half, False)
        for r2 in range(2):
            cacc[half, r2] = outs[r2]
        cst[half] = st
        axis = SECOND[half]
        me = line[axis]
        for k in ORDER:
            send(cacc.at[half], dacc.at[half, me], 8 + half, axis, k)
            send(cst.at[half], dst.at[half, me], 10 + half, axis, k)
        for r2 in range(2):
            dacc[half, me, r2] = outs[r2]
        dst[half, me] = st

    for half in range(2):
        axis = SECOND[half]
        for k in ORDER[::-1]:
            frm = peer(axis, N - k, N)
            arrived(cacc.at[half], dacc.at[half, frm], 8 + half, axis, k)
            arrived(cst.at[half], dst.at[half, frm], 10 + half, axis, k)
        outs, _ = combine(dacc, dst, half, True)
        axis = FIRST[half]
        me = line[axis]
        for r2 in range(2):
            att[me, half, r2] = outs[r2]
        for k in ORDER:
            send(att.at[me, half], att.at[me, half], 12 + half, axis, k)

    wc.wait()
    for half in range(2):
        axis = FIRST[half]
        me = line[axis]
        for k in ORDER[::-1]:
            frm = peer(axis, N - k, N)
            arrived(att.at[me, half], att.at[frm, half], 12 + half, axis, k)

    lhs = jnp.concatenate([att[o].reshape(ROWS, HD) for o in range(N)], axis=1)
    prods = []
    for h in range(KV):
        for jj in range(2):
            w = wbuf[h, :, jj].reshape(N * HD, wbuf.shape[-1])
            prods.append(jnp.dot(lhs, w, preferred_element_type=jnp.float32))
    width = wbuf.shape[-1]
    sub = lax.broadcasted_iota(jnp.int32, (8, width), 0)
    for r in range(R):
        b = r * 16
        first = jnp.where(sub < 4, prods[0][b : b + 8], prods[1][b : b + 8])
        second = jnp.where(sub < 4, prods[2][b + 8 : b + 16], prods[3][b + 8 : b + 16])
        both = first + second
        ybuf[:, r, :] = both[0:4] + both[4:8]

    xcopies = []
    for k in (2, 1, 3):
        to = peer("head", k, NX)
        copy = pltpu.make_async_remote_copy(
            src_ref=ybuf.at[to], dst_ref=xbuf.at[x], send_sem=xs.at[k - 1], recv_sem=xr.at[k - 1],
            device_id={"head": to}, device_id_type=MESH,
        )
        copy.start()
        xcopies.append((k, copy))
    result = ybuf[x]
    for c in sent:
        c.wait_send()
    for k, copy in xcopies:
        frm = peer("head", NX - k, NX)
        pltpu.make_async_remote_copy(
            src_ref=ybuf.at[0], dst_ref=xbuf.at[frm], send_sem=xs.at[k - 1], recv_sem=xr.at[k - 1],
            device_id={"head": frm}, device_id_type=MESH,
        ).wait_recv()
        result = result + xbuf[frm]
    out_ref[0] = bf16(result)
    for k, copy in xcopies:
        copy.wait_send()


def on_device(queries, key_codes, key_scale, value_codes, value_scale, out_weight, ctx_len, start_shard, draft_depth):
    width = out_weight.shape[1]
    weight = out_weight.reshape(KV, N, 2, HD, width)
    dma = pltpu.SemaphoreType.DMA
    b16, flt, i32 = jnp.bfloat16, jnp.float32, jnp.int32
    vm, sm = pltpu.VMEM, pltpu.SMEM
    return pl.pallas_call(
        kernel,
        out_shape=jax.ShapeDtypeStruct((1, R, width), b16),
        in_specs=[pl.BlockSpec(memory_space=pl.ANY)] * 9,
        out_specs=pl.BlockSpec(memory_space=pltpu.VMEM),
        scratch_shapes=[
            vm((2, N, 2, HD), b16),
            vm((2, N, 2, HD), b16),
            vm((R, N, N, 2, HD), b16),
            vm((R, KV, KEYS, HD), b16),
            vm((R, KV, KEYS, HD), b16),
            vm((KV, N, 2, HD, width), b16),
            sm((R, KV, KEYS // BLK), flt),
            sm((R, KV, KEYS // BLK), flt),
            sm((R,), i32),
            sm((R,), i32),
            sm((R, DRAFT), i32),
            vm((2, N, 2, 16, HD), b16),
            vm((2, N, 8, HD), flt),
            vm((2, N, 2, 16, HD), b16),
            vm((2, N, 8, HD), flt),
            vm((2, 2, 16, HD), b16),
            vm((2, 8, HD), flt),
            vm((2, N, 2, 16, HD), b16),
            vm((2, N, 8, HD), flt),
            vm((N, 2, 2, 16, HD), b16),
            vm((DRAFT, R, width), flt),
            vm((NX, R, width), flt),
            dma((10,)),
            dma((14, N - 1)),
            dma((14, N - 1)),
            dma((NX - 1,)),
            dma((NX - 1,)),
        ],
        compiler_params=pltpu.CompilerParams(collective_id=0, has_side_effects=True),
        name="draft_attention",
    )(queries, key_codes, key_scale, value_codes, value_scale, weight, ctx_len, start_shard, draft_depth)


def solution(mesh):
    torus = Mesh(
        mesh.devices.reshape(N, N, mesh.shape["head"], mesh.shape["req"]),
        ("seq_0", "seq_1", "head", "req"),
    )
    placed = (
        P("req", HEAD_SEQ, None),
        P("req", "head", SEQ, None),
        P("req", "head", SEQ),
        P("req", "head", SEQ, None),
        P("req", "head", SEQ),
        P("head", SEQ),
        P("req"),
        P("req"),
        P("req", None),
    )
    return jax.shard_map(
        on_device, mesh=torus, in_specs=placed, out_specs=P("head", "req", SEQ), check_vma=False
    )
```

```python
import math

import jax
import jax.numpy as jnp
from jax import lax
from jax.experimental import pallas as pl
from jax.experimental.pallas import tpu as pltpu
from jax.sharding import Mesh
from jax.sharding import PartitionSpec as P

QHEADS = 128
KVH = 8
HD = 128
DRAFT = 4
BLK = 64
SEQ = ("seq_0", "seq_1")
HEAD_SEQ = ("head", "seq_0", "seq_1")
MESH = pl.DeviceIdType.MESH

N = 8
NX = 4
R = 4
KV = 2
ROWS = 64
KEYS = 512
NEG = -1e30
FLOOR = -1e29
ORDER = (4, 3, 5, 2, 6, 1, 7)
NEAR = ORDER[::-1]
FIRST = ("seq_1", "seq_0")
SECOND = ("seq_0", "seq_1")


def peer(axis, k, size):
    return lax.rem(lax.axis_index(axis) + k, size)


def f32(x):
    return x.astype(jnp.float32)


def bf16(x):
    return x.astype(jnp.bfloat16)


def kernel(
    q_hbm, k_hbm, ks_hbm, v_hbm, vs_hbm, w_hbm, ctx_hbm, start_hbm, depth_hbm,
    out_ref,
    q0, q1, qf, kbuf, vbuf, wbuf, ks, vs, ctx, start, depth,
    krow, vrow, bias, sacc, racc, cacc, dacc, att, ybuf,
    lsem, ssem, rsem, xs, xr,
):
    y = lax.axis_index("seq_0")
    z = lax.axis_index("seq_1")
    x = lax.axis_index("head")
    line = {"seq_0": y, "seq_1": z}
    here = y * N + z

    barrier = pltpu.get_barrier_semaphore()
    for axis in SEQ:
        for k in ORDER:
            pl.semaphore_signal(barrier, inc=1, device_id={axis: peer(axis, k, N)}, device_id_type=MESH)
    for k in (2, 1, 3):
        pl.semaphore_signal(barrier, inc=1, device_id={"head": peer("head", k, NX)}, device_id_type=MESH)

    qc0 = pltpu.make_async_copy(q_hbm.at[pl.ds(0, 2)], q0.at[:, z], lsem.at[0])
    qc1 = pltpu.make_async_copy(q_hbm.at[pl.ds(2, 2)], q1.at[:, y], lsem.at[1])
    qc0.start()
    qc1.start()
    small = [
        pltpu.make_async_copy(a, b, lsem.at[2 + i])
        for i, (a, b) in enumerate(
            ((ks_hbm, ks), (vs_hbm, vs), (ctx_hbm, ctx), (start_hbm, start), (depth_hbm, depth))
        )
    ]
    for c in small:
        c.start()
    kc = pltpu.make_async_copy(k_hbm, kbuf, lsem.at[7])
    vc = pltpu.make_async_copy(v_hbm, vbuf, lsem.at[8])
    wc = pltpu.make_async_copy(w_hbm, wbuf, lsem.at[9])
    kc.start()
    vc.start()
    wc.start()
    qc0.wait()
    qc1.wait()
    pl.semaphore_wait(barrier, 2 * (N - 1) + NX - 1)

    sent = []

    def send(src, dst, slot, axis, k):
        copy = pltpu.make_async_remote_copy(
            src_ref=src, dst_ref=dst, send_sem=ssem.at[slot, k - 1], recv_sem=rsem.at[slot, k - 1],
            device_id={axis: peer(axis, k, N)}, device_id_type=MESH,
        )
        copy.start()
        sent.append(copy)

    def arrived(src, dst, slot, axis, k):
        pltpu.make_async_remote_copy(
            src_ref=src, dst_ref=dst, send_sem=ssem.at[slot, k - 1], recv_sem=rsem.at[slot, k - 1],
            device_id={axis: peer(axis, k, N)}, device_id_type=MESH,
        ).wait_recv()

    for k in ORDER:
        send(q0.at[:, z], q0.at[:, z], 0, "seq_1", k)
        send(q1.at[:, y], q1.at[:, y], 1, "seq_0", k)

    for c in small:
        c.wait()
    lane_row = lax.broadcasted_iota(jnp.int32, (1, HD), 1)
    lane_key = lax.broadcasted_iota(jnp.int32, (8, KEYS), 1)
    draft = lax.rem(lax.broadcasted_iota(jnp.int32, (8, KEYS), 0), DRAFT)
    factor = math.log2(math.e) / math.sqrt(HD)
    for r in range(R):
        offset = lax.rem(here - start[r] + N * N, N * N) * KEYS
        base = ctx[r] - DRAFT - offset
        limit = jnp.full((8, KEYS), base + depth[r, 0], jnp.int32)
        for t in range(1, DRAFT):
            limit = jnp.where(draft == t, base + depth[r, t], limit)
        bias[r] = jnp.where(lane_key <= limit, 0.0, NEG)
        for h in range(KV):
            for j in range(KEYS // HD):
                cols = pl.ds(j * HD, HD)
                krow[r, h, :, cols] = jnp.where(lane_row < BLK, ks[r, h, 2 * j], ks[r, h, 2 * j + 1]) * factor
                vrow[r, h, :, cols] = jnp.where(lane_row < BLK, vs[r, h, 2 * j], vs[r, h, 2 * j + 1])

    for k in NEAR:
        arrived(q1.at[:, y], q1.at[:, peer("seq_0", N - k, N)], 1, "seq_0", k)
    for k in ORDER:
        send(q1, qf.at[pl.ds(2, 2), :, z], 3, "seq_1", k)
    for k in NEAR:
        arrived(q0.at[:, z], q0.at[:, peer("seq_1", N - k, N)], 0, "seq_1", k)
    for k in ORDER:
        send(q0, qf.at[pl.ds(0, 2), y], 2, "seq_0", k)
    qf[0:2, y] = q0[...]
    qf[2:4, :, z] = q1[...]

    lane8 = lax.broadcasted_iota(jnp.int32, (8, HD), 1)
    row8 = lax.broadcasted_iota(jnp.int32, (8, HD), 0)
    own_lane = lax.rem(lane8, 8) == row8

    def split_rows(v):
        high = f32(bf16(v))
        rest = v - high
        mid = f32(bf16(rest))
        rows = jnp.where(row8[None] == 0, high, jnp.where(row8[None] == 1, mid, rest - mid))
        return bf16(jnp.where(row8[None] < 3, rows, 0.0))

    pick = [jnp.logical_and(own_lane, lax.div(lane8, 8) == q) for q in range(8)]

    kc.wait()
    vc.wait()
    for half in range(2):
        for k in NEAR:
            if half == 0:
                arrived(q0, qf.at[pl.ds(0, 2), peer("seq_0", N - k, N)], 2, "seq_0", k)
            else:
                arrived(q1, qf.at[pl.ds(2, 2), :, peer("seq_1", N - k, N)], 3, "seq_1", k)
        axis = FIRST[half]
        stats = jnp.zeros((N, 8, HD), jnp.float32)
        accs = {}
        for r2 in range(2):
            r = half * 2 + r2
            for h in range(KV):
                rows = qf[r, 4 * h : 4 * h + 4].reshape(ROWS, HD)
                raw = lax.dot_general(
                    rows, kbuf[r, h], (((1,), (1,)), ((), ())), preferred_element_type=jnp.float32
                )
                score = (raw * krow[r, h]).reshape(N, 8, KEYS) + bias[r][None]
                top = jnp.maximum(jnp.max(score, axis=2, keepdims=True), FLOOR)
                weight = jnp.exp2(score - top)
                total = jnp.sum(weight, axis=2, keepdims=True)
                scaled = bf16(weight.reshape(ROWS, KEYS) * vrow[r, h])
                accs[r2, h] = jnp.dot(scaled, vbuf[r, h], preferred_element_type=jnp.float32)
                c = r2 * KV + h
                stats = jnp.where(pick[c][None], top, stats)
                stats = jnp.where(pick[4 + c][None], total, stats)
        sacc[half, :, 32:40] = split_rows(jnp.sum(stats, axis=1, keepdims=True))
        for o in range(N):
            for h in range(KV):
                part = jnp.concatenate([accs[r2, h][8 * o : 8 * o + 8] for r2 in range(2)], axis=0)
                sacc[half, o, 16 * h : 16 * h + 16] = bf16(part)
        me = line[axis]
        for k in ORDER:
            send(sacc.at[half, peer(axis, k, N)], racc.at[half, me], 4 + half, axis, k)
        racc[half, me] = sacc[half, me]

    low = lane_row < 4 * 8

    def combine(accs, half, last):
        st = jnp.sum(f32(accs[half, :, 32:40]), axis=1)
        top = jnp.max(st, axis=0, keepdims=True)
        f = jnp.exp2(st - top)
        total = jnp.sum(f * pltpu.roll(st, HD - 32, 1), axis=0, keepdims=True)
        if last:
            f = f * jnp.where(low, 1.0 / total, 0.0)
        outs = [jnp.zeros((16, HD), jnp.float32) for h in range(KV)]
        for k in range(N):
            row = jnp.broadcast_to(f[k : k + 1], (8, HD))
            cols = [jnp.sum(jnp.where(pick[c], row, 0.0), axis=1, keepdims=True) for c in range(4)]
            for h in range(KV):
                w = jnp.concatenate([jnp.broadcast_to(cols[r2 * KV + h], (8, HD)) for r2 in range(2)], axis=0)
                outs[h] = outs[h] + f32(accs[half, k, 16 * h : 16 * h + 16]) * w
        return [bf16(o) for o in outs], jnp.where(low, top, pltpu.roll(total, 32, 1))

    for half in (1, 0):
        axis = FIRST[half]
        for k in NEAR:
            arrived(sacc.at[half, 0], racc.at[half, peer(axis, N - k, N)], 4 + half, axis, k)
        outs, st = combine(racc, half, False)
        for h in range(KV):
            cacc[half, 16 * h : 16 * h + 16] = outs[h]
        cacc[half, 32:40] = split_rows(st[None])[0]
        axis = SECOND[half]
        me = line[axis]
        for k in ORDER:
            send(cacc.at[half], dacc.at[half, me], 6 + half, axis, k)
        dacc[half, me] = cacc[half]

    for half in range(2):
        axis = SECOND[half]
        for k in NEAR:
            arrived(cacc.at[half], dacc.at[half, peer(axis, N - k, N)], 6 + half, axis, k)
        outs, _ = combine(dacc, half, True)
        axis = FIRST[half]
        me = line[axis]
        for h in range(KV):
            att[me, half, h] = outs[h]
        for k in ORDER:
            send(att.at[me, half], att.at[me, half], 8 + half, axis, k)

    wc.wait()
    width = wbuf.shape[-1]
    prods = [[None, None], [None, None]]

    def project(half, o):
        lhs = jnp.concatenate([att[o, half, h] for h in range(KV)], axis=1)
        for jj in range(2):
            w = jnp.concatenate([wbuf[h, o, jj] for h in range(KV)], axis=0)
            p = jnp.dot(lhs, w, preferred_element_type=jnp.float32)
            prods[half][jj] = p if prods[half][jj] is None else prods[half][jj] + p

    for half in range(2):
        project(half, line[FIRST[half]])
    for k in NEAR:
        for half in (1, 0):
            axis = FIRST[half]
            frm = peer(axis, N - k, N)
            arrived(att.at[line[axis], half], att.at[frm, half], 8 + half, axis, k)
            project(half, frm)
    sub = lax.rem(lax.broadcasted_iota(jnp.int32, (16, width), 0), 8)
    for half in range(2):
        both = jnp.where(sub < 4, prods[half][0], prods[half][1])
        for r2 in range(2):
            b = 8 * r2
            ybuf[:, 2 * half + r2, :] = both[b : b + 4] + both[b + 4 : b + 8]

    xcopies = []
    for k in (2, 1, 3):
        to = peer("head", k, NX)
        copy = pltpu.make_async_remote_copy(
            src_ref=ybuf.at[to], dst_ref=out_ref.at[x], send_sem=xs.at[k - 1], recv_sem=xr.at[k - 1],
            device_id={"head": to}, device_id_type=MESH,
        )
        copy.start()
        xcopies.append((k, copy))
    mine = pltpu.make_async_copy(ybuf.at[x], out_ref.at[x], lsem.at[0])
    mine.start()
    for c in sent:
        c.wait_send()
    mine.wait()
    for k, copy in xcopies[::-1]:
        frm = peer("head", NX - k, NX)
        pltpu.make_async_remote_copy(
            src_ref=ybuf.at[0], dst_ref=out_ref.at[frm], send_sem=xs.at[k - 1], recv_sem=xr.at[k - 1],
            device_id={"head": frm}, device_id_type=MESH,
        ).wait_recv()
    for k, copy in xcopies:
        copy.wait_send()


def on_device(queries, key_codes, key_scale, value_codes, value_scale, out_weight, ctx_len, start_shard, draft_depth):
    width = out_weight.shape[1]
    weight = out_weight.reshape(KV, N, 2, HD, width)
    dma = pltpu.SemaphoreType.DMA
    b16, flt, i32 = jnp.bfloat16, jnp.float32, jnp.int32
    vm, sm = pltpu.VMEM, pltpu.SMEM
    shares = pl.pallas_call(
        kernel,
        out_shape=jax.ShapeDtypeStruct((NX, R, width), flt),
        in_specs=[pl.BlockSpec(memory_space=pltpu.HBM)] * 9,
        out_specs=pl.BlockSpec(memory_space=pltpu.HBM),
        scratch_shapes=[
            vm((2, N, 2, HD), b16),
            vm((2, N, 2, HD), b16),
            vm((R, N, N, 2, HD), b16),
            vm((R, KV, KEYS, HD), b16),
            vm((R, KV, KEYS, HD), b16),
            vm((KV, N, 2, HD, width), b16),
            sm((R, KV, KEYS // BLK), flt),
            sm((R, KV, KEYS // BLK), flt),
            sm((R,), i32),
            sm((R,), i32),
            sm((R, DRAFT), i32),
            vm((R, KV, 1, KEYS), flt),
            vm((R, KV, 1, KEYS), flt),
            vm((R, 8, KEYS), flt),
            vm((2, N, 40, HD), b16),
            vm((2, N, 40, HD), b16),
            vm((2, 40, HD), b16),
            vm((2, N, 40, HD), b16),
            vm((N, 2, KV, 16, HD), b16),
            vm((DRAFT, R, width), flt),
            dma((10,)),
            dma((10, N - 1)),
            dma((10, N - 1)),
            dma((NX - 1,)),
            dma((NX - 1,)),
        ],
        compiler_params=pltpu.CompilerParams(collective_id=0, has_side_effects=True),
        name="draft_attention",
    )(queries, key_codes, key_scale, value_codes, value_scale, weight, ctx_len, start_shard, draft_depth)
    return bf16(jnp.sum(shares, axis=0, keepdims=True))


def solution(mesh):
    torus = Mesh(
        mesh.devices.reshape(N, N, mesh.shape["head"], mesh.shape["req"]),
        ("seq_0", "seq_1", "head", "req"),
    )
    placed = (
        P("req", HEAD_SEQ, None),
        P("req", "head", SEQ, None),
        P("req", "head", SEQ),
        P("req", "head", SEQ, None),
        P("req", "head", SEQ),
        P("head", SEQ),
        P("req"),
        P("req"),
        P("req", None),
    )
    return jax.shard_map(
        on_device, mesh=torus, in_specs=placed, out_specs=P("head", "req", SEQ), check_vma=False
    )
```
